32 devices in a mesh: blk: 16 (over z, y, core), rows: 2 (over x).
Axes of the slice: x: 2, y: 2, z: 4, core: 2. Of those that a mesh axis runs over, the one named last changes fastest.
Arguments:
- columns: float32 [2048, 1280], P('blk', 'rows'), may hold values from -9 to 9
- right_factor: float32 [2048, 512], P('blk', 'rows'), may hold values from -6 to 6
Outputs:
- new_columns: float32 [2048, 1280], P('blk', 'rows')
- new_factor: float32 [2048, 512], P('blk', 'rows')
The draws below stay inside these ranges and needn't reach their ends.
All inputs are finite; a program needn't handle non-finite values.
Results may differ from the reference program's by a relative error of at most 0.0003.
Values sent between devices are 32-bit elements; how exact they have to be, the bound alone decides.
No kernel may reach another device: no remote copies, remote signals or barrier semaphores. Data moves between devices by JAX's collectives and lax.ppermute only.
A program may use at most 64 MiB of HBM per device.

```python
import jax
import jax.numpy as jnp
from jax import lax

BLOCK = 64
STEPS = 6
ORDER = 2048
ROWS = 1280
FACTOR_ROWS = 512
N_BLK = 16


def draw_columns(key, part):
    noise_key, left_key, right_key = jax.random.split(jax.random.fold_in(key, 17), 3)
    noise_part = jax.random.truncated_normal(noise_key, -4.0, 4.0, (ORDER, ROWS), jnp.float32)
    weights = jnp.array([0.2, 0.15, 0.1, 0.07], jnp.float32)
    left_part = jax.random.truncated_normal(left_key, -3.0, 3.0, (ORDER, 4), jnp.float32) * weights
    right_part = jax.random.truncated_normal(right_key, -3.0, 3.0, (4, ROWS), jnp.float32)
    return noise_part + jnp.dot(left_part, right_part, precision=lax.Precision.HIGHEST)


def level_of(key, extent, shards, low, top_value):
    level = 1.0
    for position, shards_of in shards:
        draws = jax.random.uniform(jax.random.fold_in(jax.random.fold_in(key, 6), position), (shards_of,), jnp.float32, low / len(shards), top_value / len(shards))
        level = level * jnp.repeat(jnp.exp(draws), extent[position] // shards_of).reshape((-1,) + (1,) * (len(extent) - 1 - position))
    return level


def normal_values(rng, shape, spread, limit, cuts=(), kind=jnp.bfloat16):
    drawn = spread * jax.random.normal(rng, shape, jnp.float32)
    if cuts:
        drawn = drawn * level_of(rng, shape, cuts, -0.22, 0.18)
    return jnp.clip(drawn, -limit, limit).astype(kind)


def setup_inputs(seed: int = 0) -> dict:
    seeds = jax.random.split(jax.random.key(seed), 3)
    return {
        "columns": draw_columns(jax.random.fold_in(seeds[2], 71), 0),
        "right_factor": normal_values(seeds[1], (ORDER, FACTOR_ROWS), 1.0, 6.0, ((0, 16), (1, 2)), jnp.float32),
    }


HIGHEST_PREC = lax.Precision.HIGHEST

def orth_factor(square):
    lower_factor = jnp.linalg.cholesky(jnp.dot(square.T, square, precision=HIGHEST_PREC))
    return jax.scipy.linalg.solve_triangular(lower_factor, square.T, lower=True).T

def rotation(pair_gram):
    first_turn = orth_factor(pair_gram)
    return orth_factor(jnp.dot(pair_gram, first_turn, precision=HIGHEST_PREC))

def pass_moving(blocks):
    return jnp.concatenate([blocks[:, :BLOCK], jnp.roll(blocks[:, BLOCK:], 1, axis=0)], axis=1)

def reference(columns, right_factor):
    column_pairs = columns.reshape(N_BLK, 2 * BLOCK, ROWS)
    factor_pairs = right_factor.reshape(N_BLK, 2 * BLOCK, FACTOR_ROWS)

    def advance(current, unused):
        column_pairs, factor_pairs = current
        pair_grams = jnp.einsum('pim,pjm->pij', column_pairs, column_pairs, precision=HIGHEST_PREC)
        rotations = jax.vmap(rotation)(pair_grams)
        column_pairs = jnp.einsum('pij,pim->pjm', rotations, column_pairs, precision=HIGHEST_PREC)
        factor_pairs = jnp.einsum('pij,pim->pjm', rotations, factor_pairs, precision=HIGHEST_PREC)
        return ((pass_moving(column_pairs), pass_moving(factor_pairs)), None)
    final_state, unused = lax.scan(advance, (column_pairs, factor_pairs), None, length=STEPS)
    return (final_state[0].reshape(ORDER, ROWS), final_state[1].reshape(ORDER, FACTOR_ROWS))
```

```python
import functools

import jax
import jax.numpy as jnp
from jax import lax
from jax.experimental import pallas as pl
from jax.experimental.pallas import tpu as pltpu
from jax.sharding import PartitionSpec as P

STEPS = 6
SUB = 8
LANES = 128

HIGHEST_PREC = lax.Precision.HIGHEST


def shifted(block, axis, distance):
    size = lax.axis_size(axis)
    return lax.ppermute(block, axis, [((i - distance) % size, i) for i in range(size)])


def row_of(tile, k):
    return jnp.broadcast_to(tile[k:k + 1, :], tile.shape)


def column_of(tile, lane):
    return jnp.broadcast_to(tile[:, lane:lane + 1], tile.shape)


def tree_sum(terms):
    while len(terms) > 1:
        paired = [a + b for a, b in zip(terms[::2], terms[1::2])]
        if len(terms) % 2:
            paired.append(terms[-1])
        terms = paired
    return terms[0]


def eliminate(square, extras):
    count = len(square)
    sublane = lax.broadcasted_iota(jnp.int32, square[0].shape, 0)
    states = [list(square)] + [list(e) for e in extras]
    results = [[] for _ in states]
    for j in range(count):
        base = SUB * j
        tiles = [state[j] for state in states]
        columns = [column_of(tiles[0], base + m) for m in range(SUB)]
        scales, pivots_rows, coefficients = [], [], {}
        scale_column = None
        for k in range(SUB):
            scale = lax.rsqrt(row_of(columns[k], k))
            scales.append(scale)
            rows = [row_of(tile, k) * scale for tile in tiles]
            pivots_rows.append(rows)
            scale_column = scale if k == 0 else jnp.where(sublane == k, scale, scale_column)
            if k + 1 < SUB:
                multiplier = jnp.where(sublane > k, columns[k] * scale, 0.0)
                for m in range(k + 1, SUB):
                    coefficients[k, m] = row_of(multiplier, m)
                    columns[m] = columns[m] - multiplier * coefficients[k, m]
                tiles = [tile - multiplier * row for tile, row in zip(tiles, rows)]
        for result, tile in zip(results, tiles):
            result.append(tile * scale_column)
        for i in range(j + 1, count):
            multipliers = []
            for m in range(SUB):
                entry = column_of(states[0][i], base + m)
                for k in range(m):
                    entry = entry - multipliers[k] * coefficients[k, m]
                multipliers.append(entry * scales[m])
            for s, state in enumerate(states):
                state[i] = state[i] - tree_sum([multipliers[k] * pivots_rows[k][s] for k in range(SUB)])
    return results


def tiles_of(matrix):
    return [matrix[SUB * i:SUB * (i + 1)] for i in range(matrix.shape[0] // SUB)]


def rotation_transposed(gram):
    squared = jnp.dot(gram, gram, precision=HIGHEST_PREC)
    upper = jnp.concatenate(eliminate(tiles_of(squared), [])[0], 0)
    inner = lax.dot_general(upper, upper, (((1,), (1,)), ((), ())), precision=HIGHEST_PREC)
    return jnp.concatenate(eliminate(tiles_of(inner), [tiles_of(upper)])[1], 0)


def step_kernel(stay, moving, factor_stay, factor_moving, new_stay, new_moving, new_factor_stay, new_factor_moving):
    width = stay.shape[0]
    pair = jnp.concatenate([stay[...], moving[...]], 0)
    gram = lax.dot_general(pair, pair, (((1,), (1,)), ((), ())), precision=HIGHEST_PREC)
    turn = rotation_transposed(gram)
    rotated = jnp.dot(turn, pair, precision=HIGHEST_PREC)
    new_stay[...] = rotated[:width]
    new_moving[...] = rotated[width:]
    factor = jnp.concatenate([factor_stay[...], factor_moving[...]], 0)
    rotated_factor = jnp.dot(turn, factor, precision=HIGHEST_PREC)
    new_factor_stay[...] = rotated_factor[:width]
    new_factor_moving[...] = rotated_factor[width:]


def step(*arrays):
    return pl.pallas_call(
        step_kernel,
        out_shape=tuple(jax.ShapeDtypeStruct(a.shape, a.dtype) for a in arrays),
        name="pair_step",
    )(*arrays)


def body(columns, right_factor):
    width = columns.shape[0] // 2
    own = columns.shape[1]
    everywhere = jnp.concatenate(
        [columns] + [shifted(columns, "rows", d) for d in range(1, lax.axis_size("rows"))], 1
    )

    def advance(step_index, state):
        new = step(*state)
        return (new[0], shifted(new[1], "blk", 1), new[2], shifted(new[3], "blk", 1))

    state = (everywhere[:width], everywhere[width:], right_factor[:width], right_factor[width:])
    state = lax.fori_loop(0, STEPS, advance, state)
    return (
        jnp.concatenate([state[0][:, :own], state[1][:, :own]], 0),
        jnp.concatenate([state[2], state[3]], 0),
    )


def solution(mesh):
    return jax.shard_map(
        body,
        mesh=mesh,
        in_specs=(P("blk", "rows"), P("blk", "rows")),
        out_specs=(P("blk", "rows"), P("blk", "rows")),
        check_vma=False,
    )
```

```python
import functools

import jax
import jax.numpy as jnp
from jax import lax
from jax.experimental import pallas as pl
from jax.experimental.pallas import tpu as pltpu
from jax.sharding import PartitionSpec as P

STEPS = 6
SUB = 8
KERNEL_PARAMS = pltpu.CompilerParams(vmem_limit_bytes=24 * 1024 * 1024)

HIGHEST_PREC = lax.Precision.HIGHEST


def shifted(block, axis, distance):
    size = lax.axis_size(axis)
    return lax.ppermute(block, axis, [((i - distance) % size, i) for i in range(size)])


def row_of(tile, k):
    return jnp.broadcast_to(tile[k:k + 1, :], tile.shape)


def column_of(tile, lane):
    return jnp.broadcast_to(tile[:, lane:lane + 1], tile.shape)


def tree_sum(terms):
    while len(terms) > 1:
        paired = [a + b for a, b in zip(terms[::2], terms[1::2])]
        if len(terms) % 2:
            paired.append(terms[-1])
        terms = paired
    return terms[0]


def eliminate(square, extras):
    count = len(square)
    sublane = lax.broadcasted_iota(jnp.int32, square[0].shape, 0)
    states = [list(square)] + [list(e) for e in extras]
    results = [[] for _ in states]
    for j in range(count):
        base = SUB * j
        tiles = [state[j] for state in states]
        columns = [column_of(tiles[0], base + m) for m in range(SUB)]
        scales, pivots_rows, coefficients = [], [], {}
        scale_column = None
        for k in range(SUB):
            scale = lax.rsqrt(row_of(columns[k], k))
            scales.append(scale)
            rows = [row_of(tile, k) * scale for tile in tiles]
            pivots_rows.append(rows)
            scale_column = scale if k == 0 else jnp.where(sublane == k, scale, scale_column)
            if k + 1 < SUB:
                multiplier = jnp.where(sublane > k, columns[k] * scale, 0.0)
                for m in range(k + 1, SUB):
                    coefficients[k, m] = row_of(multiplier, m)
                    columns[m] = columns[m] - multiplier * coefficients[k, m]
                tiles = [tile - multiplier * row for tile, row in zip(tiles, rows)]
        for result, tile in zip(results, tiles):
            result.append(tile * scale_column)
        for i in range(j + 1, count):
            multipliers = []
            for m in range(SUB):
                entry = column_of(states[0][i], base + m)
                for k in range(m):
                    entry = entry - multipliers[k] * coefficients[k, m]
                multipliers.append(entry * scales[m])
            for s, state in enumerate(states):
                state[i] = state[i] - tree_sum([multipliers[k] * pivots_rows[k][s] for k in range(SUB)])
    return results


def tiles_of(matrix):
    return [matrix[SUB * i:SUB * (i + 1)] for i in range(matrix.shape[0] // SUB)]


def rotation_transposed(gram):
    squared = jnp.dot(gram, gram, precision=HIGHEST_PREC)
    upper = jnp.concatenate(eliminate(tiles_of(squared), [])[0], 0)
    inner = lax.dot_general(upper, upper, (((1,), (1,)), ((), ())), precision=HIGHEST_PREC)
    return jnp.concatenate(eliminate(tiles_of(inner), [tiles_of(upper)])[1], 0)


def split(values):
    high = values.astype(jnp.bfloat16)
    return high, (values - high.astype(jnp.float32)).astype(jnp.bfloat16)


def three_pass(left, right, dims):
    left_high, left_low = split(left)
    right_high, right_low = split(right)

    def product(a, b):
        return lax.dot_general(a, b, (dims, ((), ())), preferred_element_type=jnp.float32)

    return product(left_high, right_high) + (product(left_high, right_low) + product(left_low, right_high))


def turn_kernel(stay, moving, turn):
    pair = jnp.concatenate([stay[...], moving[...]], 0)
    turn[...] = rotation_transposed(three_pass(pair, pair, ((1,), (1,))))


def rotate_kernel(turn, upper, lower, factor_upper, factor_lower, *outputs):
    columns = jnp.concatenate([upper[...], lower[...]], 0)
    factor = jnp.concatenate([factor_upper[...], factor_lower[...]], 0)
    width = upper.shape[0]
    for index in range(len(outputs) // 2):
        rows = turn[width * index:width * (index + 1), :]
        outputs[2 * index][...] = three_pass(rows, columns, ((1,), (0,)))
        outputs[2 * index + 1][...] = three_pass(rows, factor, ((1,), (0,)))


def find_turn(stay, moving):
    size = 2 * stay.shape[0]
    return pl.pallas_call(
        turn_kernel,
        out_shape=jax.ShapeDtypeStruct((size, size), stay.dtype),
        compiler_params=KERNEL_PARAMS,
        name="find_turn",
    )(stay, moving)


def rotate(turn, upper, lower, factor_upper, factor_lower, halves):
    shapes = [jax.ShapeDtypeStruct(a.shape, a.dtype) for a in (upper, factor_upper)]
    return pl.pallas_call(
        rotate_kernel,
        out_shape=tuple(shapes * halves),
        input_output_aliases={1: 0, 3: 1},
        compiler_params=KERNEL_PARAMS,
        name=f"rotate_{halves}",
    )(turn, upper, lower, factor_upper, factor_lower)


def body(columns, right_factor):
    width = columns.shape[0] // 2
    own = columns.shape[1]
    everywhere = jnp.concatenate(
        [columns] + [shifted(columns, "rows", d) for d in range(1, lax.axis_size("rows"))], 1
    )

    def advance(step_index, state):
        stay, moving, near_stay, factor_stay, factor_moving, near_factor_stay = state
        near_moving = shifted(moving, "blk", 1)
        near_factor_moving = shifted(factor_moving, "blk", 1)
        turn = find_turn(stay, moving)
        near_turn = shifted(turn, "blk", 1)
        stay, factor_stay = rotate(turn, stay, moving, factor_stay, factor_moving, 1)
        near_stay, near_factor_stay, moving, factor_moving = rotate(
            near_turn, near_stay, near_moving, near_factor_stay, near_factor_moving, 2
        )
        return stay, moving, near_stay, factor_stay, factor_moving, near_factor_stay

    state = (
        everywhere[:width], everywhere[width:], shifted(everywhere[:width], "blk", 1),
        right_factor[:width], right_factor[width:], shifted(right_factor[:width], "blk", 1),
    )
    stay, moving, _, factor_stay, factor_moving, _ = lax.fori_loop(0, STEPS, advance, state)
    return (
        jnp.concatenate([stay[:, :own], moving[:, :own]], 0),
        jnp.concatenate([factor_stay, factor_moving], 0),
    )


def solution(mesh):
    return jax.shard_map(
        body,
        mesh=mesh,
        in_specs=(P("blk", "rows"), P("blk", "rows")),
        out_specs=(P("blk", "rows"), P("blk", "rows")),
        check_vma=False,
    )
```

```python
import functools

import jax
import jax.numpy as jnp
from jax import lax
from jax.experimental import pallas as pl
from jax.experimental.pallas import tpu as pltpu
from jax.sharding import PartitionSpec as P


STEPS = 6
SUB = 8
KERNEL_PARAMS = pltpu.CompilerParams(vmem_limit_bytes=24 * 1024 * 1024)

HIGHEST_PREC = lax.Precision.HIGHEST


def shifted(block, axis, distance):
    size = lax.axis_size(axis)
    return lax.ppermute(block, axis, [((i - distance) % size, i) for i in range(size)])


def row_of(tile, k):
    return jnp.broadcast_to(tile[k:k + 1, :], tile.shape)


def column_of(tile, lane):
    return jnp.broadcast_to(tile[:, lane:lane + 1], tile.shape)


def tree_sum(terms):
    while len(terms) > 1:
        paired = [a + b for a, b in zip(terms[::2], terms[1::2])]
        if len(terms) % 2:
            paired.append(terms[-1])
        terms = paired
    return terms[0]


def sweep(square, extras):
    count = len(square)
    sublane = lax.broadcasted_iota(jnp.int32, square[0].shape, 0)
    below = [sublane > k for k in range(SUB)]
    states = [list(square)] + [list(e) for e in extras]
    results = [[] for _ in states]
    diagonal = [column_of(states[0][0], m) for m in range(SUB)]
    for j in range(count):
        base = SUB * j
        tiles = [state[j] for state in states]
        has_next = j + 1 < count
        if has_next:
            beside = [column_of(states[0][j + 1], base + m) for m in range(SUB)]
            ahead = [column_of(states[0][j + 1], base + SUB + m) for m in range(SUB)]
        scales, pivot_rows, coefficients, multipliers, growth = [], [], {}, [], [[] for _ in range(SUB)]
        scale_column = None
        for k in range(SUB):
            lower = jnp.where(below[k], diagonal[k], 0.0)
            scale = lax.rsqrt(row_of(diagonal[k], k))
            scales.append(scale)
            rows = [row_of(tile, k) * scale for tile in tiles]
            pivot_rows.append(rows)
            scale_column = scale if k == 0 else jnp.where(sublane == k, scale, scale_column)
            if k + 1 < SUB:
                factor = lower * scale
                for m in range(k + 1, SUB):
                    entry = row_of(diagonal[k], m)
                    coefficients[k, m] = entry * scale
                    if m == k + 1:
                        diagonal[m] = diagonal[m] - (lower * entry) * (scale * scale)
                    else:
                        diagonal[m] = diagonal[m] - factor * coefficients[k, m]
                tiles = [tile - factor * row for tile, row in zip(tiles, rows)]
            if has_next:
                multiplier = beside[k] * scale
                multipliers.append(multiplier)
                for m in range(k + 1, SUB):
                    beside[m] = beside[m] - multiplier * coefficients[k, m]
                for m in range(SUB):
                    growth[m].append(multiplier * row_of(multiplier, m))
        for result, tile in zip(results, tiles):
            result.append(tile * scale_column)
        if has_next:
            diagonal = [ahead[m] - tree_sum(growth[m]) for m in range(SUB)]
            for s, state in enumerate(states):
                state[j + 1] = state[j + 1] - tree_sum([multipliers[k] * pivot_rows[k][s] for k in range(SUB)])
        for i in range(j + 2, count):
            multipliers = []
            for m in range(SUB):
                entry = column_of(states[0][i], base + m)
                for k in range(m):
                    entry = entry - multipliers[k] * coefficients[k, m]
                multipliers.append(entry * scales[m])
            for s, state in enumerate(states):
                state[i] = state[i] - tree_sum([multipliers[k] * pivot_rows[k][s] for k in range(SUB)])
    return [jnp.concatenate(result, 0) for result in results]


def tiles_of(matrix):
    return [matrix[SUB * i:SUB * (i + 1)] for i in range(matrix.shape[0] // SUB)]


def exact(left, right, left_dim, right_dim):
    return lax.dot_general(left, right, (((left_dim,), (right_dim,)), ((), ())), precision=HIGHEST_PREC)


def twice(matrix):
    return jnp.concatenate([matrix, matrix], 0)


def rotation_transposed(gram):
    half = gram.shape[0] // 2
    squared = exact(gram, gram, 1, 0)
    (top,) = sweep(tiles_of(squared[:half]), [])
    change = exact(top[:, half:], top, 0, 0)
    lower_rows = squared[half:] - change
    lower_rows = jnp.concatenate([lower_rows[:, half:], lower_rows[:, half:]], 1)
    (bottom,) = sweep(tiles_of(lower_rows), [])
    bottom = jnp.where(lax.broadcasted_iota(jnp.int32, bottom.shape, 1) >= half, bottom, 0.0)
    first = sweep(tiles_of(exact(top, twice(top), 1, 1)), [tiles_of(top)])[1]
    mixed = exact(bottom, twice(first), 1, 1)
    cross = mixed[:, :half]
    inner = exact(bottom, twice(bottom), 1, 1) - exact(cross, twice(cross), 1, 1)
    second = sweep(tiles_of(inner), [tiles_of(bottom - exact(cross, first, 1, 0))])[1]
    return jnp.concatenate([first, second], 0)


def split(values):
    high = values.astype(jnp.bfloat16)
    return high, (values - high.astype(jnp.float32)).astype(jnp.bfloat16)


def three_pass(left, right, dims):
    left_high, left_low = split(left)
    right_high, right_low = split(right)

    def product(a, b):
        return lax.dot_general(a, b, (dims, ((), ())), preferred_element_type=jnp.float32)

    return product(left_high, right_high) + (product(left_high, right_low) + product(left_low, right_high))


def gram_kernel(columns, gram):
    gram[...] = three_pass(columns[...], columns[...], ((1,), (1,)))


def first_turn_kernel(*refs):
    grams = [ref[...] for ref in refs[:-1]]
    refs[-1][...] = rotation_transposed(tree_sum(grams))


def turn_kernel(entries, stay, moving, turn):
    pair = jnp.concatenate([stay[:, :entries], moving[:, :entries]], 0)
    turn[...] = rotation_transposed(three_pass(pair, pair, ((1,), (1,))))


def rotate_kernel(turn, upper, lower, *outputs):
    pair = jnp.concatenate([upper[...], lower[...]], 0)
    width = upper.shape[0]
    for index, output in enumerate(outputs):
        output[...] = three_pass(turn[width * index:width * (index + 1), :], pair, ((1,), (0,)))


def square_call(kernel, size, *operands):
    return pl.pallas_call(
        kernel, out_shape=jax.ShapeDtypeStruct((size, size), operands[0].dtype), compiler_params=KERNEL_PARAMS
    )(*operands)


def rotate(turn, upper, lower, halves):
    return pl.pallas_call(
        rotate_kernel,
        out_shape=(jax.ShapeDtypeStruct(upper.shape, upper.dtype),) * halves,
        input_output_aliases={1: 0},
        compiler_params=KERNEL_PARAMS,
    )(turn, upper, lower)


def body(columns, right_factor):
    size, own = columns.shape
    width = size // 2
    row_devices = lax.axis_size("rows")
    others = range(1, row_devices)

    def from_near_other(block, distance):
        pairs = lax.axis_size("blk")
        route = [
            (p * row_devices + (r - distance) % row_devices, (p + 1) % pairs * row_devices + r)
            for p in range(pairs) for r in range(row_devices)
        ]
        return lax.ppermute(block, ("blk", "rows"), route)

    near_own = shifted(columns, "blk", 1)
    gram = square_call(gram_kernel, size, columns)
    grams = [gram] + [shifted(gram, "rows", d) for d in others]
    foreign = [shifted(columns, "rows", d) for d in others]
    near_factor = shifted(right_factor, "blk", 1)
    turn = square_call(first_turn_kernel, size, *grams)
    near_foreign = [from_near_other(columns, d) for d in others]
    everywhere = jnp.concatenate([columns, *foreign, right_factor], 1)
    near = jnp.concatenate([near_own, *near_foreign, near_factor], 1)

    def finish(turn, stay, moving, near_stay, near_moving):
        near_turn = shifted(turn, "blk", 1)
        (stay,) = rotate(turn, stay, moving, 1)
        near_stay, moving = rotate(near_turn, near_stay, near_moving, 2)
        return stay, moving, near_stay

    def advance(step_index, state):
        stay, moving, near_stay = state
        near_moving = shifted(moving, "blk", 1)
        turn = square_call(functools.partial(turn_kernel, own * row_devices), size, stay, moving)
        return finish(turn, stay, moving, near_stay, near_moving)

    state = finish(turn, everywhere[:width], everywhere[width:], near[:width], near[width:])
    stay, moving, _ = lax.fori_loop(1, STEPS, advance, state)
    result = jnp.concatenate([stay, moving], 0)
    return result[:, :own], result[:, own * row_devices:]


def solution(mesh):
    return jax.shard_map(
        body,
        mesh=mesh,
        in_specs=(P("blk", "rows"), P("blk", "rows")),
        out_specs=(P("blk", "rows"), P("blk", "rows")),
        check_vma=False,
    )
```

```python
import functools

import jax
import jax.numpy as jnp
from jax import lax
from jax.experimental import pallas as pl
from jax.experimental.pallas import tpu as pltpu
from jax.sharding import PartitionSpec as P


STEPS = 6
SUB = 8
KERNEL_PARAMS = pltpu.CompilerParams(vmem_limit_bytes=24 * 1024 * 1024)

HIGHEST_PREC = lax.Precision.HIGHEST


def shifted(block, axis, distance):
    size = lax.axis_size(axis)
    return lax.ppermute(block, axis, [((i - distance) % size, i) for i in range(size)])


def row_of(tile, k):
    return jnp.broadcast_to(tile[k:k + 1, :], tile.shape)


def column_of(tile, lane):
    return jnp.broadcast_to(tile[:, lane:lane + 1], tile.shape)


def tree_sum(terms):
    while len(terms) > 1:
        paired = [a + b for a, b in zip(terms[::2], terms[1::2])]
        if len(terms) % 2:
            paired.append(terms[-1])
        terms = paired
    return terms[0]


def sweep(square, extras):
    count = len(square)
    sublane = lax.broadcasted_iota(jnp.int32, square[0].shape, 0)
    below = [sublane > k for k in range(SUB)]
    states = [list(square)] + [list(e) for e in extras]
    results = [[] for _ in states]
    diagonal = [column_of(states[0][0], m) for m in range(SUB)]
    for j in range(count):
        base = SUB * j
        tiles = [state[j] for state in states]
        has_next = j + 1 < count
        if has_next:
            beside = [column_of(states[0][j + 1], base + m) for m in range(SUB)]
            ahead = [column_of(states[0][j + 1], base + SUB + m) for m in range(SUB)]
        scales, pivot_rows, coefficients, multipliers, growth = [], [], {}, [], [[] for _ in range(SUB)]
        scale_column = None
        for k in range(SUB):
            pivot = row_of(diagonal[0], 0) if k == 0 else next_pivot
            lower = jnp.where(below[k], diagonal[k], 0.0)
            scale = lax.rsqrt(pivot)
            scales.append(scale)
            if k + 1 < SUB:
                entry = row_of(diagonal[k], k + 1)
                next_pivot = row_of(diagonal[k + 1], k + 1) - (entry * entry) * (scale * scale)
            rows = [row_of(tile, k) * scale for tile in tiles]
            pivot_rows.append(rows)
            scale_column = scale if k == 0 else jnp.where(sublane == k, scale, scale_column)
            if k + 1 < SUB:
                factor = lower * scale
                for m in range(k + 1, SUB):
                    coefficients[k, m] = row_of(diagonal[k], m) * scale
                    diagonal[m] = diagonal[m] - factor * coefficients[k, m]
                tiles = [tile - factor * row for tile, row in zip(tiles, rows)]
            if has_next:
                multiplier = beside[k] * scale
                multipliers.append(multiplier)
                for m in range(k + 1, SUB):
                    beside[m] = beside[m] - multiplier * coefficients[k, m]
                for m in range(SUB):
                    growth[m].append(multiplier * row_of(multiplier, m))
        for result, tile in zip(results, tiles):
            result.append(tile * scale_column)
        if has_next:
            diagonal = [ahead[m] - tree_sum(growth[m]) for m in range(SUB)]
            for s, state in enumerate(states):
                state[j + 1] = state[j + 1] - tree_sum([multipliers[k] * pivot_rows[k][s] for k in range(SUB)])
        for i in range(j + 2, count):
            multipliers = []
            for m in range(SUB):
                entry = column_of(states[0][i], base + m)
                for k in range(m):
                    entry = entry - multipliers[k] * coefficients[k, m]
                multipliers.append(entry * scales[m])
            for s, state in enumerate(states):
                state[i] = state[i] - tree_sum([multipliers[k] * pivot_rows[k][s] for k in range(SUB)])
    return [jnp.concatenate(result, 0) for result in results]


def tiles_of(matrix):
    return [matrix[SUB * i:SUB * (i + 1)] for i in range(matrix.shape[0] // SUB)]


def exact(left, right, left_dim, right_dim):
    return lax.dot_general(left, right, (((left_dim,), (right_dim,)), ((), ())), precision=HIGHEST_PREC)


def twice(matrix):
    return jnp.concatenate([matrix, matrix], 0)


def rotation_transposed(gram):
    half = gram.shape[0] // 2
    squared = exact(gram, gram, 1, 0)
    (top,) = sweep(tiles_of(squared[:half]), [])
    change = three_pass(top[:, half:], top, ((0,), (0,)))
    lower_rows = squared[half:] - change
    lower_rows = jnp.concatenate([lower_rows[:, half:], lower_rows[:, half:]], 1)
    (bottom,) = sweep(tiles_of(lower_rows), [])
    bottom = jnp.where(lax.broadcasted_iota(jnp.int32, bottom.shape, 1) >= half, bottom, 0.0)
    first = sweep(tiles_of(exact(top, twice(top), 1, 1)), [tiles_of(top)])[1]
    cross = three_pass(bottom, first, ((1,), (1,)))
    inner = exact(bottom, twice(bottom), 1, 1) - three_pass(cross, twice(cross), ((1,), (1,)))
    second = sweep(tiles_of(inner), [tiles_of(bottom - three_pass(cross, first, ((1,), (0,))))])[1]
    return jnp.concatenate([first, second], 0)


def split(values):
    high = values.astype(jnp.bfloat16)
    return high, (values - high.astype(jnp.float32)).astype(jnp.bfloat16)


def three_pass(left, right, dims):
    left_high, left_low = split(left)
    right_high, right_low = split(right)

    def product(a, b):
        return lax.dot_general(a, b, (dims, ((), ())), preferred_element_type=jnp.float32)

    return product(left_high, right_high) + (product(left_high, right_low) + product(left_low, right_high))


def gram_kernel(columns, gram):
    gram[...] = three_pass(columns[...], columns[...], ((1,), (1,)))


def first_turn_kernel(*refs):
    grams = [ref[...] for ref in refs[:-1]]
    refs[-1][...] = rotation_transposed(tree_sum(grams))


def turn_kernel(entries, stay, moving, turn):
    pair = jnp.concatenate([stay[:, :entries], moving[:, :entries]], 0)
    turn[...] = rotation_transposed(three_pass(pair, pair, ((1,), (1,))))


def rotate_kernel(turn, upper, lower, *outputs):
    pair = jnp.concatenate([upper[...], lower[...]], 0)
    width = upper.shape[0]
    for index, output in enumerate(outputs):
        output[...] = three_pass(turn[width * index:width * (index + 1), :], pair, ((1,), (0,)))


def rotate_pieces_kernel(halves, turn, *refs):
    pieces, outputs = refs[:-halves], refs[-halves:]
    width = turn.shape[0] // 2
    start = 0
    for piece in pieces:
        stop = start + piece.shape[1]
        for index, output in enumerate(outputs):
            rows = turn[width * index:width * (index + 1), :]
            output[:, start:stop] = three_pass(rows, piece[...], ((1,), (0,)))
        start = stop


def deliver_kernel(stay, moving, new_columns, new_factor, sems):
    width = stay.shape[0]
    own = new_columns.shape[1]
    factor_at = stay.shape[1] - new_factor.shape[1]
    copies = []
    for index, block in enumerate((stay, moving)):
        rows = pl.ds(width * index, width)
        copies.append((block.at[:, pl.ds(0, own)], new_columns.at[rows, :]))
        copies.append((block.at[:, pl.ds(factor_at, new_factor.shape[1])], new_factor.at[rows, :]))
    started = [
        pltpu.make_async_copy(source, target, sems.at[n]) for n, (source, target) in enumerate(copies)
    ]
    for copy in started:
        copy.start()
    for copy in started:
        copy.wait()


def square_call(kernel, size, *operands):
    return pl.pallas_call(
        kernel, out_shape=jax.ShapeDtypeStruct((size, size), operands[0].dtype), compiler_params=KERNEL_PARAMS
    )(*operands)


def rotate(turn, upper, lower, halves):
    return pl.pallas_call(
        rotate_kernel,
        out_shape=(jax.ShapeDtypeStruct(upper.shape, upper.dtype),) * halves,
        input_output_aliases={1: 0},
        compiler_params=KERNEL_PARAMS,
    )(turn, upper, lower)


def rotate_pieces(turn, pieces, halves):
    width = turn.shape[0] // 2
    total = sum(piece.shape[1] for piece in pieces)
    return pl.pallas_call(
        functools.partial(rotate_pieces_kernel, halves),
        out_shape=(jax.ShapeDtypeStruct((width, total), turn.dtype),) * halves,
        compiler_params=KERNEL_PARAMS,
    )(turn, *pieces)


def deliver(stay, moving, own, factor_rows):
    size = 2 * stay.shape[0]
    return pl.pallas_call(
        deliver_kernel,
        out_shape=tuple(jax.ShapeDtypeStruct((size, n), stay.dtype) for n in (own, factor_rows)),
        in_specs=[pl.BlockSpec(memory_space=pltpu.VMEM)] * 2,
        out_specs=(pl.BlockSpec(memory_space=pl.ANY),) * 2,
        scratch_shapes=(pltpu.SemaphoreType.DMA((4,)),),
        compiler_params=KERNEL_PARAMS,
        name="deliver",
    )(stay, moving)


def body(columns, right_factor):
    size, own = columns.shape
    row_devices = lax.axis_size("rows")
    others = range(1, row_devices)

    def from_near_other(block, distance):
        pairs = lax.axis_size("blk")
        route = [
            (p * row_devices + (r - distance) % row_devices, (p + 1) % pairs * row_devices + r)
            for p in range(pairs) for r in range(row_devices)
        ]
        return lax.ppermute(block, ("blk", "rows"), route)

    near_own = shifted(columns, "blk", 1)
    gram = square_call(gram_kernel, size, columns)
    grams = [gram] + [shifted(gram, "rows", d) for d in others]
    foreign = [shifted(columns, "rows", d) for d in others]
    near_factor = shifted(right_factor, "blk", 1)
    turn = square_call(first_turn_kernel, size, *grams)
    near_foreign = [from_near_other(columns, d) for d in others]

    def finish(turn, stay, moving, near_stay, near_moving):
        near_turn = shifted(turn, "blk", 1)
        (stay,) = rotate(turn, stay, moving, 1)
        near_stay, moving = rotate(near_turn, near_stay, near_moving, 2)
        return stay, moving, near_stay

    def advance(step_index, state):
        stay, moving, near_stay = state
        near_moving = shifted(moving, "blk", 1)
        turn = square_call(functools.partial(turn_kernel, own * row_devices), size, stay, moving)
        return finish(turn, stay, moving, near_stay, near_moving)

    near_turn = shifted(turn, "blk", 1)
    (stay,) = rotate_pieces(turn, (columns, *foreign, right_factor), 1)
    near_stay, moving = rotate_pieces(near_turn, (near_own, *near_foreign, near_factor), 2)
    stay, moving, _ = lax.fori_loop(1, STEPS, advance, (stay, moving, near_stay))
    return deliver(stay, moving, own, right_factor.shape[1])


def solution(mesh):
    return jax.shard_map(
        body,
        mesh=mesh,
        in_specs=(P("blk", "rows"), P("blk", "rows")),
        out_specs=(P("blk", "rows"), P("blk", "rows")),
        check_vma=False,
    )
```

```python
import functools

import jax
import jax.numpy as jnp
from jax import lax
from jax.experimental import pallas as pl
from jax.experimental.pallas import tpu as pltpu
from jax.sharding import PartitionSpec as P


STEPS = 6
SUB = 8
LATE = 2
KERNEL_PARAMS = pltpu.CompilerParams(vmem_limit_bytes=24 * 1024 * 1024)

HIGHEST_PREC = lax.Precision.HIGHEST


def shifted(block, axis, distance):
    size = lax.axis_size(axis)
    return lax.ppermute(block, axis, [((i - distance) % size, i) for i in range(size)])


def row_of(tile, k):
    return jnp.broadcast_to(tile[k:k + 1, :], tile.shape)


def column_of(tile, lane):
    return jnp.broadcast_to(tile[:, lane:lane + 1], tile.shape)


def tree_sum(terms):
    while len(terms) > 1:
        paired = [a + b for a, b in zip(terms[::2], terms[1::2])]
        if len(terms) % 2:
            paired.append(terms[-1])
        terms = paired
    return terms[0]


def sweep(square, extras):
    count = len(square)
    sublane = lax.broadcasted_iota(jnp.int32, square[0].shape, 0)
    below = [sublane > k for k in range(SUB)]
    states = [list(square)] + [list(e) for e in extras]
    results = [[] for _ in states]
    diagonal = [column_of(states[0][0], m) for m in range(SUB)]
    for j in range(count):
        base = SUB * j
        tiles = [state[j] for state in states]
        has_next = j + 1 < count
        if has_next:
            beside = [column_of(states[0][j + 1], base + m) for m in range(SUB)]
            ahead = [column_of(states[0][j + 1], base + SUB + m) for m in range(SUB - LATE)]
        scales, pivot_rows, coefficients, multipliers, growth = [], [], {}, [], [[] for _ in range(SUB)]
        scale_column = None
        for k in range(SUB):
            pivot = row_of(diagonal[0], 0) if k == 0 else next_pivot
            lower = jnp.where(below[k], diagonal[k], 0.0)
            scale = lax.rsqrt(pivot)
            scales.append(scale)
            if k + 1 < SUB:
                entry = row_of(diagonal[k], k + 1)
                next_pivot = row_of(diagonal[k + 1], k + 1) - (entry * entry) * (scale * scale)
            rows = [row_of(tile, k) * scale for tile in tiles]
            pivot_rows.append(rows)
            scale_column = scale if k == 0 else jnp.where(sublane == k, scale, scale_column)
            if k + 1 < SUB:
                factor = lower * scale
                for m in range(k + 1, SUB):
                    coefficients[k, m] = row_of(diagonal[k], m) * scale
                    diagonal[m] = diagonal[m] - factor * coefficients[k, m]
                tiles = [tile - factor * row for tile, row in zip(tiles, rows)]
            if has_next:
                multiplier = beside[k] * scale
                multipliers.append(multiplier)
                for m in range(k + 1, SUB):
                    beside[m] = beside[m] - multiplier * coefficients[k, m]
                for m in range(SUB - LATE):
                    growth[m].append(multiplier * row_of(multiplier, m))
        for result, tile in zip(results, tiles):
            result.append(tile * scale_column)
        if has_next:
            diagonal = [ahead[m] - tree_sum(growth[m]) for m in range(SUB - LATE)]
            for s, state in enumerate(states):
                state[j + 1] = state[j + 1] - tree_sum([multipliers[k] * pivot_rows[k][s] for k in range(SUB)])
            diagonal += [column_of(states[0][j + 1], base + SUB + m) for m in range(SUB - LATE, SUB)]
        for i in range(j + 2, count):
            multipliers = []
            for m in range(SUB):
                entry = column_of(states[0][i], base + m)
                for k in range(m):
                    entry = entry - multipliers[k] * coefficients[k, m]
                multipliers.append(entry * scales[m])
            for s, state in enumerate(states):
                state[i] = state[i] - tree_sum([multipliers[k] * pivot_rows[k][s] for k in range(SUB)])
    return [jnp.concatenate(result, 0) for result in results]


def tiles_of(matrix):
    return [matrix[SUB * i:SUB * (i + 1)] for i in range(matrix.shape[0] // SUB)]


def parts_of(values, count):
    parts = []
    for _ in range(count - 1):
        parts.append(values.astype(jnp.bfloat16))
        values = values - parts[-1].astype(jnp.float32)
    return parts + [values.astype(jnp.bfloat16)]


def stacked(left, right, left_dim, right_dim, terms):
    count = 1 + max(max(term) for term in terms)
    lefts, rights = parts_of(left, count), parts_of(right, count)
    return lax.dot_general(
        jnp.concatenate([lefts[a] for a, _ in terms], left_dim),
        jnp.concatenate([rights[b] for _, b in terms], right_dim),
        (((left_dim,), (right_dim,)), ((), ())),
        preferred_element_type=jnp.float32,
    )


THREE_TERMS = ((0, 1), (1, 0), (0, 0))


def exact(left, right, left_dim, right_dim):
    return lax.dot_general(left, right, (((left_dim,), (right_dim,)), ((), ())), precision=HIGHEST_PREC)


def twice(matrix):
    return jnp.concatenate([matrix, matrix], 0)


def rotation_transposed(gram):
    half = gram.shape[0] // 2
    squared = exact(gram, gram, 1, 0)
    (top,) = sweep(tiles_of(squared[:half]), [])
    change = stacked(top, top, 0, 0, THREE_TERMS)
    lower_rows = squared[half:] - change[half:]
    lower_rows = jnp.concatenate([lower_rows[:, half:], lower_rows[:, half:]], 1)
    (bottom,) = sweep(tiles_of(lower_rows), [])
    bottom = jnp.where(lax.broadcasted_iota(jnp.int32, bottom.shape, 1) >= half, bottom, 0.0)
    first = sweep(tiles_of(exact(top, twice(top), 1, 1)), [tiles_of(top)])[1]
    cross = stacked(bottom, first, 1, 1, THREE_TERMS)
    inner = exact(bottom, twice(bottom), 1, 1) - three_pass(cross, twice(cross), ((1,), (1,)))
    second = sweep(tiles_of(inner), [tiles_of(bottom - three_pass(cross, first, ((1,), (0,))))])[1]
    return jnp.concatenate([first, second], 0)


def split(values):
    high = values.astype(jnp.bfloat16)
    return high, (values - high.astype(jnp.float32)).astype(jnp.bfloat16)


def three_pass(left, right, dims):
    left_high, left_low = split(left)
    right_high, right_low = split(right)

    def product(a, b):
        return lax.dot_general(a, b, (dims, ((), ())), preferred_element_type=jnp.float32)

    return product(left_high, right_high) + (product(left_high, right_low) + product(left_low, right_high))


def gram_of(pair):
    high, low = split(pair)
    size = pair.shape[0]
    both = lax.dot_general(
        jnp.concatenate([low, high], 0), high, (((1,), (1,)), ((), ())), preferred_element_type=jnp.float32
    )
    return both[size:] + (both[:size] + both[:size].T)


def gram_kernel(columns, gram):
    gram[...] = gram_of(columns[...])


def first_turn_kernel(*refs):
    grams = [ref[...] for ref in refs[:-1]]
    refs[-1][...] = rotation_transposed(tree_sum(grams))


def turn_kernel(entries, stay, moving, turn):
    pair = jnp.concatenate([stay[:, :entries], moving[:, :entries]], 0)
    turn[...] = rotation_transposed(gram_of(pair))


def turned(rows, values):
    rows_high, rows_low = split(rows)
    high, low = split(values)

    def product(a, b):
        return jnp.dot(a, b, preferred_element_type=jnp.float32)

    both = product(jnp.concatenate([rows_high, rows_high], 1), jnp.concatenate([high, low], 0))
    return both + product(rows_low, high)


def rotate_kernel(turn, upper, lower, *outputs):
    pair = jnp.concatenate([upper[...], lower[...]], 0)
    width = upper.shape[0]
    rotated = turned(turn[:width * len(outputs), :], pair)
    for index, output in enumerate(outputs):
        output[...] = rotated[width * index:width * (index + 1)]


def rotate_pieces_kernel(halves, turn, *refs):
    pieces, outputs = refs[:-halves], refs[-halves:]
    width = turn.shape[0] // 2
    start = 0
    for piece in pieces:
        stop = start + piece.shape[1]
        for index, output in enumerate(outputs):
            rows = turn[width * index:width * (index + 1), :]
            output[:, start:stop] = three_pass(rows, piece[...], ((1,), (0,)))
        start = stop


def deliver_kernel(stay, moving, new_columns, new_factor, sems):
    width = stay.shape[0]
    own = new_columns.shape[1]
    factor_at = stay.shape[1] - new_factor.shape[1]
    copies = []
    for index, block in enumerate((stay, moving)):
        rows = pl.ds(width * index, width)
        copies.append((block.at[:, pl.ds(0, own)], new_columns.at[rows, :]))
        copies.append((block.at[:, pl.ds(factor_at, new_factor.shape[1])], new_factor.at[rows, :]))
    started = [
        pltpu.make_async_copy(source, target, sems.at[n]) for n, (source, target) in enumerate(copies)
    ]
    for copy in started:
        copy.start()
    for copy in started:
        copy.wait()


def square_call(kernel, size, *operands):
    return pl.pallas_call(
        kernel, out_shape=jax.ShapeDtypeStruct((size, size), operands[0].dtype), compiler_params=KERNEL_PARAMS
    )(*operands)


def rotate(turn, upper, lower, halves):
    return pl.pallas_call(
        rotate_kernel,
        out_shape=(jax.ShapeDtypeStruct(upper.shape, upper.dtype),) * halves,
        input_output_aliases={1: 0},
        compiler_params=KERNEL_PARAMS,
    )(turn, upper, lower)


def rotate_pieces(turn, pieces, halves):
    width = turn.shape[0] // 2
    total = sum(piece.shape[1] for piece in pieces)
    return pl.pallas_call(
        functools.partial(rotate_pieces_kernel, halves),
        out_shape=(jax.ShapeDtypeStruct((width, total), turn.dtype),) * halves,
        compiler_params=KERNEL_PARAMS,
    )(turn, *pieces)


def deliver(stay, moving, own, factor_rows):
    size = 2 * stay.shape[0]
    return pl.pallas_call(
        deliver_kernel,
        out_shape=tuple(jax.ShapeDtypeStruct((size, n), stay.dtype) for n in (own, factor_rows)),
        in_specs=[pl.BlockSpec(memory_space=pltpu.VMEM)] * 2,
        out_specs=(pl.BlockSpec(memory_space=pl.ANY),) * 2,
        scratch_shapes=(pltpu.SemaphoreType.DMA((4,)),),
        compiler_params=KERNEL_PARAMS,
        name="deliver",
    )(stay, moving)


def body(columns, right_factor):
    size, own = columns.shape
    row_devices = lax.axis_size("rows")
    others = range(1, row_devices)

    def from_near_other(block, distance):
        pairs = lax.axis_size("blk")
        route = [
            (p * row_devices + (r - distance) % row_devices, (p + 1) % pairs * row_devices + r)
            for p in range(pairs) for r in range(row_devices)
        ]
        return lax.ppermute(block, ("blk", "rows"), route)

    near_own = shifted(columns, "blk", 1)
    gram = square_call(gram_kernel, size, columns)
    grams = [gram] + [shifted(gram, "rows", d) for d in others]
    foreign = [shifted(columns, "rows", d) for d in others]
    near_factor = shifted(right_factor, "blk", 1)
    turn = square_call(first_turn_kernel, size, *grams)
    near_foreign = [from_near_other(columns, d) for d in others]

    def finish(turn, stay, moving, near_stay, near_moving):
        near_turn = shifted(turn, "blk", 1)
        (stay,) = rotate(turn, stay, moving, 1)
        near_stay, moving = rotate(near_turn, near_stay, near_moving, 2)
        return stay, moving, near_stay

    def advance(step_index, state):
        stay, moving, near_stay = state
        near_moving = shifted(moving, "blk", 1)
        turn = square_call(functools.partial(turn_kernel, own * row_devices), size, stay, moving)
        return finish(turn, stay, moving, near_stay, near_moving)

    near_turn = shifted(turn, "blk", 1)
    (stay,) = rotate_pieces(turn, (columns, *foreign, right_factor), 1)
    near_stay, moving = rotate_pieces(near_turn, (near_own, *near_foreign, near_factor), 2)
    stay, moving, _ = lax.fori_loop(1, STEPS, advance, (stay, moving, near_stay))
    return deliver(stay, moving, own, right_factor.shape[1])


def solution(mesh):
    return jax.shard_map(
        body,
        mesh=mesh,
        in_specs=(P("blk", "rows"), P("blk", "rows")),
        out_specs=(P("blk", "rows"), P("blk", "rows")),
        check_vma=False,
    )
```

```python
import functools

import jax
import jax.numpy as jnp
from jax import lax
from jax.experimental import pallas as pl
from jax.experimental.pallas import tpu as pltpu
from jax.sharding import PartitionSpec as P


STEPS = 6
SUB = 8
LATE = 2
KERNEL_PARAMS = pltpu.CompilerParams(vmem_limit_bytes=24 * 1024 * 1024)

HIGHEST_PREC = lax.Precision.HIGHEST


def shifted(block, axis, distance):
    size = lax.axis_size(axis)
    return lax.ppermute(block, axis, [((i - distance) % size, i) for i in range(size)])


def row_of(tile, k):
    return jnp.broadcast_to(tile[k:k + 1, :], tile.shape)


def column_of(tile, lane):
    return jnp.broadcast_to(tile[:, lane:lane + 1], tile.shape)


def tree_sum(terms):
    while len(terms) > 1:
        paired = [a + b for a, b in zip(terms[::2], terms[1::2])]
        if len(terms) % 2:
            paired.append(terms[-1])
        terms = paired
    return terms[0]


def sweep(square, extras):
    count = len(square)
    sublane = lax.broadcasted_iota(jnp.int32, square[0].shape, 0)
    below = [sublane > k for k in range(SUB)]
    states = [list(square)] + [list(e) for e in extras]
    results = [[] for _ in states]
    diagonal = [column_of(states[0][0], m) for m in range(SUB)]
    for j in range(count):
        base = SUB * j
        tiles = [state[j] for state in states]
        has_next = j + 1 < count
        if has_next:
            beside = [column_of(states[0][j + 1], base + m) for m in range(SUB)]
            ahead = [column_of(states[0][j + 1], base + SUB + m) for m in range(SUB - LATE)]
        scales, pivot_rows, coefficients, multipliers, growth = [], [], {}, [], [[] for _ in range(SUB)]
        scale_column = None
        for k in range(SUB):
            pivot = row_of(diagonal[0], 0) if k == 0 else next_pivot
            lower = jnp.where(below[k], diagonal[k], 0.0)
            scale = lax.rsqrt(pivot)
            scales.append(scale)
            if k + 1 < SUB:
                entry = row_of(diagonal[k], k + 1)
                next_pivot = row_of(diagonal[k + 1], k + 1) - (entry * entry) * (scale * scale)
            rows = [row_of(tile, k) * scale for tile in tiles]
            pivot_rows.append(rows)
            scale_column = scale if k == 0 else jnp.where(sublane == k, scale, scale_column)
            if k + 1 < SUB:
                factor = lower * scale
                for m in range(k + 1, SUB):
                    coefficients[k, m] = row_of(diagonal[k], m) * scale
                    diagonal[m] = diagonal[m] - factor * coefficients[k, m]
                tiles = [tile - factor * row for tile, row in zip(tiles, rows)]
            if has_next:
                multiplier = beside[k] * scale
                multipliers.append(multiplier)
                for m in range(k + 1, SUB):
                    beside[m] = beside[m] - multiplier * coefficients[k, m]
                for m in range(SUB - LATE):
                    growth[m].append(multiplier * row_of(multiplier, m))
        for result, tile in zip(results, tiles):
            result.append(tile * scale_column)
        if has_next:
            diagonal = [ahead[m] - tree_sum(growth[m]) for m in range(SUB - LATE)]
            for s, state in enumerate(states):
                state[j + 1] = state[j + 1] - tree_sum([multipliers[k] * pivot_rows[k][s] for k in range(SUB)])
            diagonal += [column_of(states[0][j + 1], base + SUB + m) for m in range(SUB - LATE, SUB)]
        for i in range(j + 2, count):
            multipliers = []
            for m in range(SUB):
                entry = column_of(states[0][i], base + m)
                for k in range(m):
                    entry = entry - multipliers[k] * coefficients[k, m]
                multipliers.append(entry * scales[m])
            for s, state in enumerate(states):
                state[i] = state[i] - tree_sum([multipliers[k] * pivot_rows[k][s] for k in range(SUB)])
    return [jnp.concatenate(result, 0) for result in results]


def tiles_of(matrix):
    return [matrix[SUB * i:SUB * (i + 1)] for i in range(matrix.shape[0] // SUB)]


def parts_of(values, count):
    parts = []
    for _ in range(count - 1):
        parts.append(values.astype(jnp.bfloat16))
        values = values - parts[-1].astype(jnp.float32)
    return parts + [values.astype(jnp.bfloat16)]


def stacked(left, right, left_dim, right_dim, terms):
    count = 1 + max(max(term) for term in terms)
    lefts, rights = parts_of(left, count), parts_of(right, count)
    return lax.dot_general(
        jnp.concatenate([lefts[a] for a, _ in terms], left_dim),
        jnp.concatenate([rights[b] for _, b in terms], right_dim),
        (((left_dim,), (right_dim,)), ((), ())),
        preferred_element_type=jnp.float32,
    )


SIX_TERMS = ((0, 2), (2, 0), (1, 1), (0, 1), (1, 0), (0, 0))


def exact(left, right, left_dim, right_dim):
    return lax.dot_general(left, right, (((left_dim,), (right_dim,)), ((), ())), precision=HIGHEST_PREC)


def twice(matrix):
    return jnp.concatenate([matrix, matrix], 0)


def rotation_transposed(gram):
    half = gram.shape[0] // 2
    squared = exact(gram, gram, 1, 0)
    (top,) = sweep(tiles_of(squared[:half]), [])
    change = stacked(top, top, 0, 0, SIX_TERMS)
    lower_rows = squared[half:] - change[half:]
    lower_rows = jnp.concatenate([lower_rows[:, half:], lower_rows[:, half:]], 1)
    (bottom,) = sweep(tiles_of(lower_rows), [])
    bottom = jnp.where(lax.broadcasted_iota(jnp.int32, bottom.shape, 1) >= half, bottom, 0.0)
    first = sweep(tiles_of(exact(top, twice(top), 1, 1)), [tiles_of(top)])[1]
    cross = stacked(bottom, first, 1, 1, SIX_TERMS)
    inner = exact(bottom, twice(bottom), 1, 1) - exact(cross, twice(cross), 1, 1)
    second = sweep(tiles_of(inner), [tiles_of(bottom - exact(cross, first, 1, 0))])[1]
    return jnp.concatenate([first, second], 0)


def split(values):
    high = values.astype(jnp.bfloat16)
    return high, (values - high.astype(jnp.float32)).astype(jnp.bfloat16)


def gram_of(pair):
    high, low = split(pair)
    size = pair.shape[0]
    both = lax.dot_general(
        jnp.concatenate([low, high], 0), high, (((1,), (1,)), ((), ())), preferred_element_type=jnp.float32
    )
    return both[size:] + (both[:size] + both[:size].T)


def gram_kernel(columns, gram):
    gram[...] = gram_of(columns[...])


def first_turn_kernel(*refs):
    grams = [ref[...] for ref in refs[:-1]]
    refs[-1][...] = rotation_transposed(tree_sum(grams))


def turn_kernel(entries, stay, moving, turn):
    pair = jnp.concatenate([stay[:, :entries], moving[:, :entries]], 0)
    turn[...] = rotation_transposed(gram_of(pair))


def turned(rows, values):
    return stacked(rows, values, 1, 0, SIX_TERMS)


def rotate_kernel(turn, upper, lower, *outputs):
    pair = jnp.concatenate([upper[...], lower[...]], 0)
    width = upper.shape[0]
    rotated = turned(turn[:width * len(outputs), :], pair)
    for index, output in enumerate(outputs):
        output[...] = rotated[width * index:width * (index + 1)]


def rotate_pieces_kernel(halves, turn, *refs):
    pieces, outputs = refs[:-halves], refs[-halves:]
    width = turn.shape[0] // 2
    start = 0
    for piece in pieces:
        stop = start + piece.shape[1]
        for index, output in enumerate(outputs):
            output[:, start:stop] = turned(turn[width * index:width * (index + 1), :], piece[...])
        start = stop


def deliver_kernel(stay, moving, new_columns, new_factor, sems):
    width = stay.shape[0]
    own = new_columns.shape[1]
    factor_at = stay.shape[1] - new_factor.shape[1]
    copies = []
    for index, block in enumerate((stay, moving)):
        rows = pl.ds(width * index, width)
        copies.append((block.at[:, pl.ds(0, own)], new_columns.at[rows, :]))
        copies.append((block.at[:, pl.ds(factor_at, new_factor.shape[1])], new_factor.at[rows, :]))
    started = [
        pltpu.make_async_copy(source, target, sems.at[n]) for n, (source, target) in enumerate(copies)
    ]
    for copy in started:
        copy.start()
    for copy in started:
        copy.wait()


def square_call(kernel, size, *operands):
    return pl.pallas_call(
        kernel, out_shape=jax.ShapeDtypeStruct((size, size), operands[0].dtype), compiler_params=KERNEL_PARAMS
    )(*operands)


def rotate(turn, upper, lower, halves):
    return pl.pallas_call(
        rotate_kernel,
        out_shape=(jax.ShapeDtypeStruct(upper.shape, upper.dtype),) * halves,
        input_output_aliases={1: 0},
        compiler_params=KERNEL_PARAMS,
    )(turn, upper, lower)


def rotate_pieces(turn, pieces, halves):
    width = turn.shape[0] // 2
    total = sum(piece.shape[1] for piece in pieces)
    return pl.pallas_call(
        functools.partial(rotate_pieces_kernel, halves),
        out_shape=(jax.ShapeDtypeStruct((width, total), turn.dtype),) * halves,
        compiler_params=KERNEL_PARAMS,
    )(turn, *pieces)


def deliver(stay, moving, own, factor_rows):
    size = 2 * stay.shape[0]
    return pl.pallas_call(
        deliver_kernel,
        out_shape=tuple(jax.ShapeDtypeStruct((size, n), stay.dtype) for n in (own, factor_rows)),
        in_specs=[pl.BlockSpec(memory_space=pltpu.VMEM)] * 2,
        out_specs=(pl.BlockSpec(memory_space=pl.ANY),) * 2,
        scratch_shapes=(pltpu.SemaphoreType.DMA((4,)),),
        compiler_params=KERNEL_PARAMS,
        name="deliver",
    )(stay, moving)


def body(columns, right_factor):
    size, own = columns.shape
    row_devices = lax.axis_size("rows")
    others = range(1, row_devices)

    def from_near_other(block, distance):
        pairs = lax.axis_size("blk")
        route = [
            (p * row_devices + (r - distance) % row_devices, (p + 1) % pairs * row_devices + r)
            for p in range(pairs) for r in range(row_devices)
        ]
        return lax.ppermute(block, ("blk", "rows"), route)

    near_own = shifted(columns, "blk", 1)
    gram = square_call(gram_kernel, size, columns)
    grams = [gram] + [shifted(gram, "rows", d) for d in others]
    foreign = [shifted(columns, "rows", d) for d in others]
    near_factor = shifted(right_factor, "blk", 1)
    turn = square_call(first_turn_kernel, size, *grams)
    near_foreign = [from_near_other(columns, d) for d in others]

    def finish(turn, stay, moving, near_stay, near_moving):
        near_turn = shifted(turn, "blk", 1)
        (stay,) = rotate(turn, stay, moving, 1)
        near_stay, moving = rotate(near_turn, near_stay, near_moving, 2)
        return stay, moving, near_stay

    def advance(step_index, state):
        stay, moving, near_stay = state
        near_moving = shifted(moving, "blk", 1)
        turn = square_call(functools.partial(turn_kernel, own * row_devices), size, stay, moving)
        return finish(turn, stay, moving, near_stay, near_moving)

    near_turn = shifted(turn, "blk", 1)
    (stay,) = rotate_pieces(turn, (columns, *foreign, right_factor), 1)
    near_stay, moving = rotate_pieces(near_turn, (near_own, *near_foreign, near_factor), 2)
    stay, moving, _ = lax.fori_loop(1, STEPS, advance, (stay, moving, near_stay))
    return deliver(stay, moving, own, right_factor.shape[1])


def solution(mesh):
    return jax.shard_map(
        body,
        mesh=mesh,
        in_specs=(P("blk", "rows"), P("blk", "rows")),
        out_specs=(P("blk", "rows"), P("blk", "rows")),
        check_vma=False,
    )
```
